64 devices in a mesh: data: 4 (over x, y), stage: 16 (over z, core).
Axes of the slice: x: 2, y: 2, z: 8, core: 2. Of those that a mesh axis runs over, the one named last changes fastest.
The devices are a block of a 4x4x8 slice.
Arguments:
- x_init: float32 [4, 256, 16], P('data'), parts along dimension 0
- h_warm: bfloat16 [15, 4, 256, 768], P(None, 'data'), parts along dimension 1
- w_lat: bfloat16 [16, 16, 768], P('stage')
- w_qkv: bfloat16 [16, 768, 2304], P('stage')
- w_o: bfloat16 [16, 12, 64, 768], P('stage')
- w_up: bfloat16 [16, 768, 3072], P('stage')
- w_down: bfloat16 [16, 3072, 768], P('stage')
- w_out: bfloat16 [768, 16], replicated
- ada_mods: float32 [4, 16, 6, 768], P(None, 'stage')
- alpha_coef: float32 [4], replicated
- beta_coef: float32 [4], replicated
Outputs:
- output 1: float32 [4, 256, 16], P('data'), parts along dimension 0
- output 2: bfloat16 [16, 4, 256, 768], P('stage', 'data'), parts along dimension 1
There are 4 independent parts. The reference program is written for one: setup_inputs(seed, part) draws one part's arguments, and reference() takes and returns one part's arrays. A program takes and returns all parts, laid end to end along the dimension named above; an argument that names none is the same for every part.
All inputs are finite; a program needn't handle non-finite values.
Results may differ from the reference program's by a relative error of at most 0.0153327.
Values are sent between devices in bfloat16 or wider.
A program may use at most 768 MiB of HBM per device.

```python
import jax
import jax.numpy as jnp
from jax import lax

D = 768
HEADS = 12
TOKENS = 256
CH = 16
BATCH = 1
BLOCKS_STAGE = 1
STEPS = 4
STAGES = 16

LAYERS = STAGES * BLOCKS_STAGE
HEAD = D // HEADS


def setup_inputs(seed: int = 0, part: int = 0) -> dict:
    shared_keys = jax.random.split(jax.random.key(seed), 9)
    part_keys = jax.random.split(jax.random.fold_in(jax.random.key(seed + 1), part), 2)
    x_init = jax.random.normal(part_keys[0], (BATCH, TOKENS, CH), jnp.float32)
    h_warm = jax.random.normal(part_keys[1], (STAGES - 1, BATCH, TOKENS, D), jnp.float32).astype(jnp.bfloat16)
    w_lat = (jax.random.normal(shared_keys[0], (STAGES, CH, D), jnp.float32) * CH ** -0.5).astype(jnp.bfloat16)
    w_qkv = (jax.random.normal(shared_keys[1], (LAYERS, D, 3 * D), jnp.float32) * (1.5 * D ** -0.5)).astype(jnp.bfloat16)
    w_o = (jax.random.normal(shared_keys[2], (LAYERS, HEADS, HEAD, D), jnp.float32) * D ** -0.5).astype(jnp.bfloat16)
    w_up = (jax.random.normal(shared_keys[3], (LAYERS, D, 4 * D), jnp.float32) * D ** -0.5).astype(jnp.bfloat16)
    w_down = (jax.random.normal(shared_keys[4], (LAYERS, 4 * D, D), jnp.float32) * (4 * D) ** -0.5).astype(jnp.bfloat16)
    w_out = (jax.random.normal(shared_keys[5], (D, CH), jnp.float32) * D ** -0.5).astype(jnp.bfloat16)
    mod_base = jnp.array([0.0, 0.0, 1.0, 0.0, 0.0, 0.6], jnp.float32)[:, None]
    ada_mods = mod_base + 0.3 * jax.random.normal(shared_keys[6], (STEPS, LAYERS, 6, D), jnp.float32)
    alpha_coef = jax.random.uniform(shared_keys[7], (STEPS,), jnp.float32, 0.7, 1.0)
    beta_coef = -jax.random.uniform(shared_keys[8], (STEPS,), jnp.float32, 0.3, 0.6)
    return {'x_init': x_init, 'h_warm': h_warm, 'w_lat': w_lat, 'w_qkv': w_qkv, 'w_o': w_o, 'w_up': w_up, 'w_down': w_down, 'w_out': w_out, 'ada_mods': ada_mods, 'alpha_coef': alpha_coef, 'beta_coef': beta_coef}


def layer_norm(h_cur):
    row_mean = jnp.mean(h_cur, axis=-1, keepdims=True)
    centered = h_cur - row_mean
    row_var = jnp.mean(centered * centered, axis=-1, keepdims=True)
    return centered * lax.rsqrt(row_var + 1e-6)


def dit_block(h_cur, w_qkv, w_o, w_up, w_down, mod_vec):
    batch_size, tokens = h_cur.shape[0], h_cur.shape[1]
    u_attn = (layer_norm(h_cur) * (1.0 + mod_vec[1]) + mod_vec[0]).astype(jnp.bfloat16)
    qkv_proj = jnp.einsum('bnd,de->bne', u_attn.astype(jnp.float32), w_qkv.astype(jnp.float32)).astype(jnp.bfloat16)
    qkv_proj = qkv_proj.reshape(batch_size, tokens, 3, HEADS, HEAD).astype(jnp.float32)
    scores = jnp.einsum('bqhd,bkhd->bhqk', qkv_proj[:, :, 0], qkv_proj[:, :, 1]) * HEAD ** -0.5
    attn_probs = jax.nn.softmax(scores, axis=-1).astype(jnp.bfloat16).astype(jnp.float32)
    attn_out = jnp.einsum('bhqk,bkhd->bqhd', attn_probs, qkv_proj[:, :, 2]).astype(jnp.bfloat16).astype(jnp.float32)
    h_cur = h_cur + mod_vec[2] * jnp.einsum('bqhd,hde->bqe', attn_out, w_o.astype(jnp.float32))
    u_mlp = (layer_norm(h_cur) * (1.0 + mod_vec[4]) + mod_vec[3]).astype(jnp.bfloat16)
    hidden = jax.nn.gelu(jnp.einsum('bnd,df->bnf', u_mlp.astype(jnp.float32), w_up.astype(jnp.float32)), approximate=True).astype(jnp.bfloat16)
    return h_cur + mod_vec[5] * jnp.einsum('bnf,fd->bnd', hidden.astype(jnp.float32), w_down.astype(jnp.float32))


def run_stage(h_cur, weights_s, mods_s):
    def one_block(carry_h, block_in):
        w_qkv, w_o, w_up, w_down, mod_vec = block_in
        return dit_block(carry_h, w_qkv, w_o, w_up, w_down, mod_vec), None
    h_out, _ = lax.scan(one_block, h_cur, weights_s + (mods_s,))
    return h_out


def reference(x_init, h_warm, w_lat, w_qkv, w_o, w_up, w_down, w_out, ada_mods, alpha_coef, beta_coef):
    stage_w = tuple(weight.reshape((STAGES, BLOCKS_STAGE) + weight.shape[1:]) for weight in (w_qkv, w_o, w_up, w_down))
    stage_mods = ada_mods.reshape(STEPS, STAGES, BLOCKS_STAGE, 6, D)
    zero_slot = jnp.zeros((1, BATCH, TOKENS, D), jnp.bfloat16)
    prev_init = jnp.concatenate([h_warm, zero_slot], axis=0)

    def one_step(carry, step_in):
        x_cur, prev_out = carry
        mods_t, alpha_t, beta_t = step_in
        stale_in = jnp.concatenate([zero_slot, prev_out[:-1]], axis=0)
        x_lat = x_cur.astype(jnp.bfloat16).astype(jnp.float32)

        def one_stage(stage_in):
            stale_s, lat_s, weights_s, mods_s = stage_in
            h_cur = stale_s.astype(jnp.float32) + jnp.einsum('bnc,cd->bnd', x_lat, lat_s.astype(jnp.float32))
            return run_stage(h_cur, weights_s, mods_s).astype(jnp.bfloat16)

        stage_out = lax.map(one_stage, (stale_in, w_lat, stage_w, mods_t))
        eps_pred = jnp.einsum('bnd,dc->bnc', stage_out[STAGES - 1].astype(jnp.float32), w_out.astype(jnp.float32))
        x_next = alpha_t * x_cur + beta_t * eps_pred
        return (x_next, stage_out), None

    (x_final, last_out), _ = lax.scan(one_step, (x_init, prev_init), (stage_mods, alpha_coef, beta_coef))
    return x_final, last_out
```

```python
import functools
import math

import jax
import jax.numpy as jnp
from jax import lax
from jax.experimental import pallas as pl
from jax.experimental.pallas import tpu as pltpu
from jax.sharding import PartitionSpec as P

MESH = pl.DeviceIdType.MESH
F32, BF16 = jnp.float32, jnp.bfloat16
LANES = 128
TILE = 256
EXP2_SCALE = math.log2(math.e)
GELU_A = math.sqrt(2.0 / math.pi)
GELU_B = GELU_A * 0.044715


def normed(h_rows, scale_row, shift_row):
    width = h_rows.shape[-1]
    centered = h_rows - jnp.sum(h_rows, axis=-1, keepdims=True) * (1.0 / width)
    row_var = jnp.sum(centered * centered, axis=-1, keepdims=True) * (1.0 / width)
    return (centered * lax.rsqrt(row_var + 1e-6) * (1.0 + scale_row) + shift_row).astype(BF16)


def gelu(val):
    half = 0.5 * val
    return half * jnp.tanh(val * (GELU_B * (val * val) + GELU_A)) + half


def dot(lhs, rhs):
    return jnp.dot(lhs, rhs, preferred_element_type=F32)


def dot_t(lhs, rhs):
    return lax.dot_general(lhs, rhs, (((1,), (1,)), ((), ())), preferred_element_type=F32)


def kernel(stages, head_dim, x_hbm, warm_hbm, lat_hbm, qkv_hbm, o_hbm, up_hbm, down_hbm, out_hbm, ada_hbm, alpha_ref, beta_ref,
           xo_ref, last_hbm,
           x_f, x_b, b_in, s_out, h_ref, u_ref, qkv_ref, p_ref, v_ref, a_ref, hid_ref, x_fin,
           w_lat, w_qkv, w_o, w_up, w_down, w_out, ada,
           load_sem, b_send, b_recv, x_send, x_recv, last_sem):
    steps = alpha_ref.shape[0]
    tokens, width = h_ref.shape
    me = lax.axis_index('stage')
    is_last = me == stages - 1

    def peer(idx):
        return {'stage': idx}

    loads = {}
    for idx, (name, src, dst) in enumerate((
            ('warm', warm_hbm.at[jnp.maximum(me - 1, 0), 0], b_in.at[0]),
            ('x', x_hbm.at[0], x_f),
            ('lat', lat_hbm.at[0], w_lat),
            ('ada', ada_hbm, ada),
            ('qkv', qkv_hbm.at[0], w_qkv),
            ('o', o_hbm.at[0], w_o),
            ('up', up_hbm.at[0], w_up),
            ('down', down_hbm.at[0], w_down),
            ('out', out_hbm, w_out))):
        loads[name] = pltpu.make_async_copy(src, dst, load_sem.at[idx])
        loads[name].start()

    barrier = pltpu.get_barrier_semaphore()

    def greet(idx):
        pl.semaphore_signal(barrier, inc=1, device_id=peer(idx), device_id_type=MESH)

    @pl.when(is_last)
    def _():
        for idx in range(stages - 1):
            greet(idx)

    @pl.when(jnp.logical_not(is_last))
    def _():
        greet(stages - 1)

        @pl.when(me > 0)
        def _():
            greet(me - 1)

        @pl.when(me < stages - 2)
        def _():
            greet(me + 1)

    def send_b(step):
        return pltpu.make_async_remote_copy(s_out.at[step], b_in.at[step + 1], b_send.at[step], b_recv.at[step],
                                            device_id=peer(me + 1), device_id_type=MESH)

    def send_x(step, idx):
        return pltpu.make_async_remote_copy(x_b.at[step + 1], x_b.at[step + 1], x_send.at[idx], x_recv.at[step],
                                            device_id=peer(idx), device_id_type=MESH)

    def send_final(idx):
        return pltpu.make_async_remote_copy(x_fin, x_fin, x_send.at[idx], x_recv.at[steps - 1],
                                            device_id=peer(idx), device_id_type=MESH)

    loads['warm'].wait()

    @pl.when(me == 0)
    def _():
        for step in range(steps):
            b_in[step] = jnp.zeros((tokens, width), BF16)

    loads['x'].wait()
    loads['lat'].wait()
    loads['ada'].wait()
    x_b[0] = x_f[...].astype(BF16)

    def one_step(step, carry):
        @pl.when(jnp.logical_and(step > 0, jnp.logical_not(is_last)))
        def _():
            send_x(step - 1, 0).wait_recv()

        @pl.when(jnp.logical_and(step > 0, me > 0))
        def _():
            send_b(step - 1).wait_recv()

        def row(kind):
            return ada[step, kind]

        for r in range(0, tokens, 64):
            h_rows = b_in[step, r:r + 64, :].astype(F32) + lax.dot_general(
                x_b[step, :, r:r + 64], w_lat[...], (((0,), (0,)), ((), ())), preferred_element_type=F32)
            h_ref[r:r + 64, :] = h_rows
            u_ref[r:r + 64, :] = normed(h_rows, row(1), row(0))

        @pl.when(step == 0)
        def _():
            loads['qkv'].wait()

        for col in range(0, 3 * width, TILE):
            qkv_ref[:, col:col + TILE] = dot(u_ref[...], w_qkv[:, col:col + TILE]).astype(BF16)

        per_group = TILE // head_dim
        lane_head = lax.broadcasted_iota(jnp.int32, (1, TILE), 1) // head_dim
        for col in range(0, width, TILE):
            keys = qkv_ref[:, width + col:width + col + TILE]
            for j in range(per_group):
                mine = lane_head == j
                v_ref[j * tokens:(j + 1) * tokens, :] = jnp.where(
                    mine, qkv_ref[:, 2 * width + col:2 * width + col + TILE], 0.0).astype(BF16)
                query = jnp.where(mine, qkv_ref[:, col:col + TILE], 0.0).astype(BF16)
                scores = dot_t(query, keys)
                top = jnp.max(scores, axis=-1, keepdims=True)
                expd = jnp.exp2((scores - top) * (EXP2_SCALE * head_dim ** -0.5))
                total = jnp.sum(expd, axis=-1, keepdims=True)
                p_ref[:, j * tokens:(j + 1) * tokens] = (expd * (1.0 / total)).astype(BF16)
            a_ref[:, col:col + TILE] = dot(p_ref[...], v_ref[...]).astype(BF16)

        @pl.when(step == 0)
        def _():
            loads['o'].wait()

        for col in range(0, width, TILE):
            cols = slice(col, col + TILE)
            h_ref[:, cols] += row(2)[:, cols] * dot(a_ref[...], w_o[:, cols])
        for r in range(0, tokens, 64):
            u_ref[r:r + 64, :] = normed(h_ref[r:r + 64, :], row(4), row(3))

        @pl.when(step == 0)
        def _():
            loads['up'].wait()

        for col in range(0, w_up.shape[1], TILE):
            hid_ref[:, col:col + TILE] = gelu(dot(u_ref[...], w_up[:, col:col + TILE])).astype(BF16)

        @pl.when(step == 0)
        def _():
            loads['down'].wait()
            loads['out'].wait()

        for col in range(0, width, TILE):
            cols = slice(col, col + TILE)
            s_out[step, :, cols] = (h_ref[:, cols] + row(5)[:, cols] * dot(hid_ref[...], w_down[:, cols])).astype(BF16)

        @pl.when(step == 0)
        def _():
            pl.semaphore_wait(barrier, jnp.where(is_last, stages - 1, jnp.where(me == 0, 2, jnp.where(me == stages - 2, 2, 3))))

        @pl.when(jnp.logical_and(step < steps - 1, jnp.logical_not(is_last)))
        def _():
            send_b(step).start()

        @pl.when(is_last)
        def _():
            @pl.when(step > 0)
            def _():
                for idx in range(stages - 1):
                    send_x(step - 1, idx).wait_send()

            x_new = alpha_ref[step] * x_f[...] + beta_ref[step] * dot_t(w_out[...], s_out[step])
            x_f[...] = x_new

            @pl.when(step < steps - 1)
            def _():
                x_b[step + 1] = x_new.astype(BF16)
                for idx in range(stages - 1):
                    send_x(step, idx).start()

            @pl.when(step == steps - 1)
            def _():
                x_fin[...] = x_new
                for idx in range(stages - 1):
                    send_final(idx).start()

        return carry

    lax.fori_loop(0, steps, one_step, 0)

    put = pltpu.make_async_copy(s_out.at[steps - 1], last_hbm.at[0, 0], last_sem)
    put.start()

    @pl.when(jnp.logical_not(is_last))
    def _():
        for step in range(steps - 1):
            send_b(step).wait_send()
        send_final(0).wait_recv()

    @pl.when(is_last)
    def _():
        for idx in range(stages - 1):
            send_final(idx).wait_send()

    xo_ref[0] = x_fin[...]
    put.wait()


def solution(mesh):
    stages = mesh.shape['stage']

    def stage_program(x_init, h_warm, w_lat, w_qkv, w_o, w_up, w_down, w_out, ada_mods, alpha_coef, beta_coef):
        _, tokens, chans = x_init.shape
        width = h_warm.shape[-1]
        hidden = w_up.shape[-1]
        steps = ada_mods.shape[0]
        inner = w_o.shape[1] * w_o.shape[2]
        x_t = jnp.swapaxes(x_init, 1, 2)
        o_flat = w_o.reshape(w_o.shape[0], inner, width)
        ada = jnp.swapaxes(ada_mods, 1, 2)
        anywhere = pl.BlockSpec(memory_space=pl.ANY)
        scalars = pl.BlockSpec(memory_space=pltpu.SMEM)
        vmem = pltpu.VMEM
        dma = pltpu.SemaphoreType.DMA
        x_out, last = pl.pallas_call(
            functools.partial(kernel, stages, w_o.shape[2]),
            out_shape=(jax.ShapeDtypeStruct((1, chans, tokens), F32),
                       jax.ShapeDtypeStruct((1, 1, tokens, width), BF16)),
            in_specs=[anywhere] * 9 + [scalars] * 2,
            out_specs=(pl.BlockSpec(memory_space=vmem), anywhere),
            scratch_shapes=[
                vmem((chans, tokens), F32),
                vmem((steps, chans, tokens), BF16),
                vmem((steps, tokens, width), BF16),
                vmem((steps, tokens, width), BF16),
                vmem((tokens, width), F32),
                vmem((tokens, width), BF16),
                vmem((tokens, 3 * width), BF16),
                vmem((tokens, 4 * tokens), BF16),
                vmem((4 * tokens, TILE), BF16),
                vmem((tokens, width), BF16),
                vmem((tokens, hidden), BF16),
                vmem((chans, tokens), F32),
                vmem(w_lat.shape[1:], BF16),
                vmem(w_qkv.shape[1:], BF16),
                vmem((inner, width), BF16),
                vmem(w_up.shape[1:], BF16),
                vmem(w_down.shape[1:], BF16),
                vmem((chans, width), BF16),
                vmem(ada.shape, F32),
                dma((9,)),
                dma((steps,)),
                dma((steps,)),
                dma((stages,)),
                dma((steps,)),
                dma,
            ],
            compiler_params=pltpu.CompilerParams(collective_id=0, has_side_effects=True, vmem_limit_bytes=60 << 20),
        )(x_t, h_warm, w_lat, w_qkv, o_flat, w_up, w_down, w_out.T, ada, alpha_coef, beta_coef)
        return jnp.swapaxes(x_out, 1, 2), last

    return jax.shard_map(stage_program, mesh=mesh,
                         in_specs=(P('data'), P(None, 'data'), P('stage'), P('stage'), P('stage'), P('stage'), P('stage'), P(), P(None, 'stage'), P(), P()),
                         out_specs=(P('data'), P('stage', 'data')), check_vma=False)
```
